1024 devices in a mesh: rep: 128 (over x, z), shard: 8 (over y, core).
Axes of the slice: x: 4, y: 4, z: 32, core: 2. Of those that a mesh axis runs over, the one named last changes fastest.
Arguments:
- grads: bfloat16 [128, 24, 512, 512], P('rep', 'shard')
- owner_slot: int32 [24], replicated, may hold values from 0 to 23, as said below
- refresh: int32 [1], replicated, may hold values from 0 to 23
- left_stat: float32 [24, 512, 512], P('shard', 'rep'), as said below
- right_stat: float32 [24, 512, 512], P('shard', 'rep'), as said below
- left_root: bfloat16 [24, 512, 512], P('shard', 'rep'), as said below
- right_root: bfloat16 [24, 512, 512], P('shard'), as said below
Outputs:
- left_new: float32 [24, 512, 512], P('shard', 'rep')
- right_new: float32 [24, 512, 512], P('shard', 'rep')
- left_root_new: bfloat16 [24, 512, 512], P('shard', 'rep')
- right_root_new: bfloat16 [24, 512, 512], P('shard')
- direction: bfloat16 [24, 512, 512], P('shard')
The draws below stay inside these ranges and needn't reach their ends.
Inputs may be any that keep to these rules, and one draw needn't show every extreme that they name: A permutation: block b sits at position owner_slot[b] of owner order, which belongs to shard index owner_slot[b] // 3, with owner_slot[b] % 3 == b % 3; the 3 blocks s * 3 to s * 3 + 2 all go to different shard indices. `left_stat`: each block is symmetric positive definite. `right_stat`: each block is symmetric positive definite. `left_root`: each block is symmetric. `right_root`: each block is symmetric.
All inputs are finite; a program needn't handle non-finite values.
Results may differ from the reference program's by a relative error of at most 0.0004.
The reference program's roundings to bfloat16 on the way count: a program that leaves them out, or rounds other values in their place, can miss the bound.
Values may be sent and summed in bfloat16 or wider, within the bound.
No kernel may reach another device: no remote copies, remote signals or barrier semaphores. Data moves between devices by JAX's collectives and lax.ppermute only.
A program may use at most 32 MiB of HBM per device.

```python
import jax
import jax.numpy as jnp
from jax import lax

BS = 512
BPS = 3
ITERS = 2
REFRESH = 1
NBLK = 24
N_REP = 128
N_SHARD = 8


def draw_grads(key, part):
    key_each = jax.random.fold_in(jax.random.fold_in(key, 3), 2)
    replica_keys = jax.random.split(key_each, N_REP)

    def one_replica(replica_key):
        return (jax.random.normal(replica_key, (NBLK, BS, BS)) * (1.0 / N_REP ** 0.5)).astype(jnp.bfloat16)
    return lax.map(one_replica, replica_keys)


def draw_owner_slot(key, part):
    key_outer, key_inner, key_shift = jax.random.split(jax.random.fold_in(key, 5), 3)
    outer_perm = jax.random.permutation(key_outer, N_SHARD)
    inner_perm = jax.random.permutation(key_inner, N_SHARD)
    shift_perm = jax.random.permutation(key_shift, N_SHARD)[:BPS]
    owners = outer_perm[(inner_perm[:, None] + shift_perm[None, :]) % N_SHARD]
    slot_ids = owners * BPS + jnp.arange(BPS, dtype=jnp.int32)[None, :]
    return slot_ids.reshape(-1).astype(jnp.int32)


def stat_blocks(key):
    key_base, key_scale = jax.random.split(key)
    factor_keys = jax.random.split(key_base, NBLK)
    identity = jnp.eye(BS, dtype=jnp.float32)

    def one_block(block_key):
        normal_part = jax.random.normal(block_key, (BS, BS))
        return jnp.dot(normal_part, normal_part.T) / BS + 0.5 * identity
    blocks = lax.map(one_block, factor_keys)
    row_scale = jnp.exp(jax.random.uniform(key_scale, (NBLK, BS, 1), minval=0.0, maxval=1.15))
    return blocks * row_scale * jnp.swapaxes(row_scale, 1, 2)


def root_blocks(key):
    key_diag, key_off = jax.random.split(key)
    diagonal_part = jnp.exp(jax.random.uniform(key_diag, (NBLK, BS), minval=-0.69, maxval=0.69))
    off_part = jax.random.normal(key_off, (NBLK, BS, BS)) * (0.7 / BS ** 0.5)
    symmetric = (off_part + jnp.swapaxes(off_part, 1, 2)) * 0.5
    return (symmetric + diagonal_part[:, :, None] * jnp.eye(BS, dtype=jnp.float32)).astype(jnp.bfloat16)


def draw_left_stat(key, part):
    return stat_blocks(jax.random.fold_in(key, 11))


def draw_right_stat(key, part):
    return stat_blocks(jax.random.fold_in(key, 13))


def draw_left_root(key, part):
    return root_blocks(jax.random.fold_in(key, 17))


def draw_right_root(key, part):
    return root_blocks(jax.random.fold_in(key, 19))


def setup_inputs(seed: int = 0) -> dict:
    key_of = jax.random.split(jax.random.key(seed), 8)
    grads = draw_grads(jax.random.fold_in(key_of[7], 71), 0)
    owner_slot = draw_owner_slot(jax.random.fold_in(key_of[7], 71), 0)
    refresh = jax.random.randint(key_of[2], (REFRESH,), 0, NBLK).astype(jnp.int32)
    left_stat = draw_left_stat(jax.random.fold_in(key_of[7], 71), 0)
    right_stat = draw_right_stat(jax.random.fold_in(key_of[7], 71), 0)
    left_root = draw_left_root(jax.random.fold_in(key_of[7], 71), 0)
    right_root = draw_right_root(jax.random.fold_in(key_of[7], 71), 0)
    return dict(grads=grads, owner_slot=owner_slot, refresh=refresh, left_stat=left_stat, right_stat=right_stat, left_root=left_root, right_root=right_root)


decay_rate = 0.95
epsilon_shift = 1e-06

def inverse_root(statistic):
    order = statistic.shape[0]
    identity = jnp.eye(order, dtype=jnp.float32)
    shifted = statistic + epsilon_shift * identity
    norm_scale = 2.5 / jnp.sqrt(jnp.sum(shifted * shifted))
    moment = norm_scale * shifted
    current = identity
    for number in range(ITERS):
        factor = (5.0 * identity - moment) * 0.25
        factor_low = factor.astype(jnp.bfloat16)
        if number == 0:
            current = jnp.sqrt(jnp.sqrt(norm_scale)) * factor
        else:
            current = jnp.dot(current.astype(jnp.bfloat16), factor_low, preferred_element_type=jnp.float32)
        if number + 1 < ITERS:
            square = jnp.dot(factor_low, factor_low, preferred_element_type=jnp.float32).astype(jnp.bfloat16)
            fourth = jnp.dot(square, square, preferred_element_type=jnp.float32).astype(jnp.bfloat16)
            moment = jnp.dot(fourth, moment.astype(jnp.bfloat16), preferred_element_type=jnp.float32)
    return current.astype(jnp.bfloat16)

def add_replica(running, piece):
    return (running + piece.astype(jnp.float32), None)

def reference(grads, owner_slot, refresh, left_stat, right_stat, left_root, right_root):
    summed, unused = lax.scan(add_replica, jnp.zeros((NBLK, BS, BS), jnp.float32), grads)
    gradient = summed.astype(jnp.bfloat16)
    owned_grad = jnp.zeros_like(gradient).at[owner_slot].set(gradient)
    owned_wide = owned_grad.astype(jnp.float32)
    highest = lax.Precision.HIGHEST
    left_new = decay_rate * left_stat + jnp.einsum('bij,bkj->bik', owned_wide, owned_wide, precision=highest) / BS
    right_new = decay_rate * right_stat + jnp.einsum('bji,bjk->bik', owned_wide, owned_wide, precision=highest) / BS
    fresh_slot = owner_slot[refresh[0]]
    fresh_left = inverse_root(left_new[fresh_slot])
    fresh_right = inverse_root(right_new[fresh_slot])
    left_root_new = left_root.at[fresh_slot].set(fresh_left)
    right_root_new = right_root.at[fresh_slot].set(fresh_right)
    half_step = jnp.einsum('bij,bjk->bik', left_root_new.astype(jnp.float32), owned_wide, precision=highest).astype(jnp.bfloat16)
    direction = jnp.einsum('bij,bjk->bik', half_step.astype(jnp.float32), right_root_new.astype(jnp.float32), precision=highest).astype(jnp.bfloat16)
    return (left_new, right_new, left_root_new, right_root_new, direction)
```

```python
import jax
import jax.numpy as jnp
from jax import lax
from jax.sharding import Mesh
from jax.sharding import PartitionSpec as P

ITERS = 2
FAR, NEAR = 8, 4
Z = ("far", "near")
REP = ("x",) + Z

decay_rate = 0.95
epsilon_shift = 1e-06


def exchange(blocks, axis):
    return lax.all_to_all(blocks, axis, split_axis=0, concat_axis=0, tiled=True)


def spread(piece, axis):
    copies = jnp.broadcast_to(piece[None], (lax.axis_size(axis), *piece.shape))
    return exchange(lax.optimization_barrier(copies), axis)


def inverse_root(statistic):
    order = statistic.shape[0]
    identity = jnp.eye(order, dtype=jnp.float32)
    shifted = statistic + epsilon_shift * identity
    norm_scale = 2.5 / jnp.sqrt(jnp.sum(shifted * shifted))
    moment = norm_scale * shifted
    current = identity
    for number in range(ITERS):
        factor = (5.0 * identity - moment) * 0.25
        factor_low = factor.astype(jnp.bfloat16)
        if number == 0:
            current = jnp.sqrt(jnp.sqrt(norm_scale)) * factor
        else:
            current = jnp.dot(
                current.astype(jnp.bfloat16), factor_low, preferred_element_type=jnp.float32
            )
        if number + 1 < ITERS:
            square = jnp.dot(factor_low, factor_low, preferred_element_type=jnp.float32).astype(
                jnp.bfloat16
            )
            fourth = jnp.dot(square, square, preferred_element_type=jnp.float32).astype(
                jnp.bfloat16
            )
            moment = jnp.dot(
                fourth, moment.astype(jnp.bfloat16), preferred_element_type=jnp.float32
            )
    return current.astype(jnp.bfloat16)


def body(grads, owner_slot, refresh, left_stat, right_stat, left_root, right_root):
    blocks, order = grads.shape[1], grads.shape[2]
    xs = lax.axis_size("x")
    shards = lax.axis_size("shard")
    rows = order // (xs * FAR * NEAR)
    rep_index = lax.axis_index(REP)
    shard_index = lax.axis_index("shard")
    f32, bf16 = jnp.float32, jnp.bfloat16

    fresh_slot = owner_slot[refresh[0]]
    holder = fresh_slot // blocks
    slot_index = fresh_slot % blocks
    owns_fresh = holder == shard_index

    early = jnp.concatenate(
        [
            left_root.astype(f32),
            lax.dynamic_slice_in_dim(left_stat, slot_index, 1, 0),
            lax.dynamic_slice_in_dim(right_stat, slot_index, 1, 0),
        ]
    )
    early = spread(early, "x")
    early = lax.all_gather(early, Z)

    parts = grads[0].reshape(blocks, xs, order // xs, order).transpose(1, 0, 2, 3)
    parts = exchange(parts, "x").astype(f32)
    partial = parts[0] + parts[1] + parts[2] + parts[3]
    partial = partial.reshape(blocks, FAR, NEAR, rows, order).transpose(2, 0, 1, 3, 4)
    partial = jnp.sum(exchange(partial, "near"), axis=0)
    partial = jnp.sum(exchange(partial.transpose(1, 0, 2, 3), "far"), axis=0)
    row_share = partial.astype(bf16)

    slot_table = owner_slot.reshape(shards, blocks)
    own_slots = lax.dynamic_index_in_dim(slot_table, shard_index, 0, keepdims=False)
    targets = own_slots // blocks
    selector = (targets[None, :] == jnp.arange(shards, dtype=jnp.int32)[:, None]).astype(bf16)
    outgoing = jnp.einsum("ok,krc->orc", selector, row_share, preferred_element_type=f32)
    incoming = exchange(outgoing.astype(bf16), "shard")
    wanted = shard_index * blocks + jnp.arange(blocks, dtype=jnp.int32)
    receiver = (jnp.transpose(slot_table) == wanted[:, None]).astype(bf16)
    owned_rows = jnp.einsum("ks,src->krc", receiver, incoming, preferred_element_type=f32)
    owned_rows = owned_rows.astype(bf16)

    gathered = spread(spread(spread(owned_rows, "far"), "near"), "x")
    gathered = gathered.transpose(3, 0, 2, 1, 4, 5).reshape(blocks, order, order)

    left_new = (
        decay_rate * left_stat
        + jnp.einsum("krc,kjc->krj", owned_rows, gathered, preferred_element_type=f32) / order
    )
    column_share = lax.dynamic_slice_in_dim(gathered, rep_index * rows, rows, 2)
    right_new = (
        decay_rate * right_stat
        + jnp.einsum("kic,kij->kcj", column_share, gathered, preferred_element_type=f32) / order
    )

    early = early.transpose(2, 1, 0, 3, 4).reshape(blocks + 2, order, order)
    left_whole = early[:blocks].astype(bf16)

    def renewed(_):
        block = lax.dynamic_index_in_dim(gathered, slot_index, 0, keepdims=False)
        left = jnp.einsum("rc,jc->rj", block, block, preferred_element_type=f32) / order
        right = jnp.einsum("ic,ij->cj", block, block, preferred_element_type=f32) / order
        left_x = inverse_root(decay_rate * early[blocks] + left)
        right_x = inverse_root(decay_rate * early[blocks + 1] + right)
        rows_x = lax.dynamic_slice_in_dim(left_x, rep_index * rows, rows, 0)
        return (
            lax.dynamic_update_index_in_dim(left_root, rows_x, slot_index, 0),
            lax.dynamic_update_index_in_dim(left_whole, left_x, slot_index, 0),
            lax.dynamic_update_index_in_dim(right_root, right_x, slot_index, 0),
        )

    def kept(_):
        return (left_root, left_whole, right_root)

    left_root_new, left_whole, right_root_new = lax.cond(owns_fresh, renewed, kept, 0)
    half = jnp.einsum("kri,kic->krc", left_whole, gathered, preferred_element_type=f32).astype(bf16)
    direction = jnp.einsum("kri,kic->krc", half, right_root_new, preferred_element_type=f32)
    return (left_new, right_new, left_root_new, right_root_new, direction.astype(bf16))


def solution(mesh):
    shards = mesh.shape["shard"]
    finer = Mesh(mesh.devices.reshape(-1, FAR, NEAR, shards), (*REP, "shard"))
    whole = P("shard", None, None)
    split = P("shard", REP, None)
    in_specs = (P(REP, "shard", None, None), P(), P(), split, split, split, whole)
    out_specs = (split, split, split, whole, whole)
    return jax.shard_map(body, mesh=finer, in_specs=in_specs, out_specs=out_specs, check_vma=False)
```

```python
import jax
import jax.numpy as jnp
from jax import lax
from jax.sharding import Mesh
from jax.sharding import PartitionSpec as P

ITERS = 2
FAR, NEAR = 8, 4
Z = ("far", "near")
REP = ("x",) + Z

decay_rate = 0.95
epsilon_shift = 1e-06


def exchange(blocks, axis):
    return lax.all_to_all(blocks, axis, split_axis=0, concat_axis=0, tiled=True)


def spread(piece, axis):
    copies = jnp.broadcast_to(piece[None], (lax.axis_size(axis), *piece.shape))
    return exchange(lax.optimization_barrier(copies), axis)


def in_thirds(wide):
    high = lax.reduce_precision(wide, 8, 7)
    middle = lax.reduce_precision(wide - high, 8, 7)
    low = wide - high - middle
    return [part.astype(jnp.bfloat16) for part in (high, middle, low)]


def inverse_root(statistic):
    order = statistic.shape[0]
    identity = jnp.eye(order, dtype=jnp.float32)
    shifted = statistic + epsilon_shift * identity
    norm_scale = 2.5 / jnp.sqrt(jnp.sum(shifted * shifted))
    moment = norm_scale * shifted
    current = identity
    for number in range(ITERS):
        factor = (5.0 * identity - moment) * 0.25
        factor_low = factor.astype(jnp.bfloat16)
        if number == 0:
            current = jnp.sqrt(jnp.sqrt(norm_scale)) * factor
        else:
            current = jnp.dot(
                current.astype(jnp.bfloat16), factor_low, preferred_element_type=jnp.float32
            )
        if number + 1 < ITERS:
            square = jnp.dot(factor_low, factor_low, preferred_element_type=jnp.float32).astype(
                jnp.bfloat16
            )
            fourth = jnp.dot(square, square, preferred_element_type=jnp.float32).astype(
                jnp.bfloat16
            )
            moment = jnp.dot(
                fourth, moment.astype(jnp.bfloat16), preferred_element_type=jnp.float32
            )
    return current.astype(jnp.bfloat16)


def body(grads, owner_slot, refresh, left_stat, right_stat, left_root, right_root):
    blocks, order = grads.shape[1], grads.shape[2]
    xs = lax.axis_size("x")
    shards = lax.axis_size("shard")
    rows = order // (xs * FAR * NEAR)
    rep_index = lax.axis_index(REP)
    shard_index = lax.axis_index("shard")
    f32, bf16 = jnp.float32, jnp.bfloat16

    fresh_slot = owner_slot[refresh[0]]
    holder = fresh_slot // blocks
    slot_index = fresh_slot % blocks
    owns_fresh = holder == shard_index

    early = jnp.concatenate(
        [
            left_root,
            *in_thirds(lax.dynamic_slice_in_dim(left_stat, slot_index, 1, 0)),
            *in_thirds(lax.dynamic_slice_in_dim(right_stat, slot_index, 1, 0)),
        ]
    )
    entries = early.shape[0]
    early = jnp.broadcast_to(early.reshape(1, entries * rows, order), (xs, entries * rows, order))

    depth = order // xs
    parts = grads[0].reshape(blocks, xs, depth, order).transpose(1, 0, 2, 3)
    parts = jnp.concatenate([parts.reshape(xs, blocks * depth, order), early], axis=1)
    parts = exchange(lax.optimization_barrier(parts), "x")
    early = parts[:, blocks * depth :].reshape(xs, entries, rows, order)
    early = lax.all_gather(early, Z)
    parts = parts[:, : blocks * depth].astype(f32)
    partial = parts[0] + parts[1] + parts[2] + parts[3]
    partial = partial.reshape(blocks, FAR, NEAR, rows, order).transpose(2, 0, 1, 3, 4)
    partial = jnp.sum(exchange(partial, "near"), axis=0)
    partial = jnp.sum(exchange(partial.transpose(1, 0, 2, 3), "far"), axis=0)
    row_share = partial.astype(bf16)

    slot_table = owner_slot.reshape(shards, blocks)
    own_slots = lax.dynamic_index_in_dim(slot_table, shard_index, 0, keepdims=False)
    targets = own_slots // blocks
    selector = (targets[None, :] == jnp.arange(shards, dtype=jnp.int32)[:, None]).astype(bf16)
    outgoing = jnp.einsum("ok,krc->orc", selector, row_share, preferred_element_type=f32)
    incoming = exchange(outgoing.astype(bf16), "shard")
    wanted = shard_index * blocks + jnp.arange(blocks, dtype=jnp.int32)
    receiver = (jnp.transpose(slot_table) == wanted[:, None]).astype(bf16)
    owned_rows = jnp.einsum("ks,src->krc", receiver, incoming, preferred_element_type=f32)
    owned_rows = owned_rows.astype(bf16)

    gathered = spread(spread(spread(owned_rows, "far"), "near"), "x")
    gathered = gathered.transpose(3, 0, 2, 1, 4, 5).reshape(blocks, order, order)

    left_new = (
        decay_rate * left_stat
        + jnp.einsum("krc,kjc->krj", owned_rows, gathered, preferred_element_type=f32) / order
    )
    column_share = lax.dynamic_slice_in_dim(gathered, rep_index * rows, rows, 2)
    right_new = (
        decay_rate * right_stat
        + jnp.einsum("kic,kij->kcj", column_share, gathered, preferred_element_type=f32) / order
    )

    stats = early[:, :, blocks:].astype(f32)
    stats = stats.reshape(*stats.shape[:2], 2, 3, rows, order)
    stats = stats[:, :, :, 0] + (stats[:, :, :, 1] + stats[:, :, :, 2])
    stats = stats.transpose(2, 1, 0, 3, 4).reshape(2, order, order)
    left_whole = early[:, :, :blocks].transpose(2, 1, 0, 3, 4).reshape(blocks, order, order)

    def renewed(_):
        block = lax.dynamic_index_in_dim(gathered, slot_index, 0, keepdims=False)
        left = jnp.einsum("rc,jc->rj", block, block, preferred_element_type=f32) / order
        right = jnp.einsum("ic,ij->cj", block, block, preferred_element_type=f32) / order
        left_x = inverse_root(decay_rate * stats[0] + left)
        right_x = inverse_root(decay_rate * stats[1] + right)
        rows_x = lax.dynamic_slice_in_dim(left_x, rep_index * rows, rows, 0)
        return (
            lax.dynamic_update_index_in_dim(left_root, rows_x, slot_index, 0),
            lax.dynamic_update_index_in_dim(left_whole, left_x, slot_index, 0),
            lax.dynamic_update_index_in_dim(right_root, right_x, slot_index, 0),
        )

    def kept(_):
        return (left_root, left_whole, right_root)

    left_root_new, left_whole, right_root_new = lax.cond(owns_fresh, renewed, kept, 0)
    half = jnp.einsum("kri,kic->krc", left_whole, gathered, preferred_element_type=f32).astype(bf16)
    direction = jnp.einsum("kri,kic->krc", half, right_root_new, preferred_element_type=f32)
    return (left_new, right_new, left_root_new, right_root_new, direction.astype(bf16))


def solution(mesh):
    shards = mesh.shape["shard"]
    finer = Mesh(mesh.devices.reshape(-1, FAR, NEAR, shards), (*REP, "shard"))
    whole = P("shard", None, None)
    split = P("shard", REP, None)
    in_specs = (P(REP, "shard", None, None), P(), P(), split, split, split, whole)
    out_specs = (split, split, split, whole, whole)
    return jax.shard_map(body, mesh=finer, in_specs=in_specs, out_specs=out_specs, check_vma=False)
```

```python
import jax
import jax.numpy as jnp
from jax import lax
from jax.experimental import pallas as pl
from jax.experimental.pallas import tpu as pltpu
from jax.sharding import Mesh
from jax.sharding import PartitionSpec as P

ITERS = 2
FAR, NEAR = 8, 4
Z = ("far", "near")
REP = ("x",) + Z

decay_rate = 0.95
epsilon_shift = 1e-06


def exchange(blocks, axis):
    return lax.all_to_all(blocks, axis, split_axis=0, concat_axis=0, tiled=True)


def spread(piece, axis):
    copies = jnp.broadcast_to(piece[None], (lax.axis_size(axis), *piece.shape))
    return exchange(lax.optimization_barrier(copies), axis)


def in_halves(wide):
    high = lax.reduce_precision(wide, 8, 7)
    return [part.astype(jnp.bfloat16) for part in (high, wide - high)]


def inverse_root(statistic):
    order = statistic.shape[0]
    row = lax.broadcasted_iota(jnp.int32, statistic.shape, 0)
    column = lax.broadcasted_iota(jnp.int32, statistic.shape, 1)
    identity = (row == column).astype(jnp.float32)
    shifted = statistic + epsilon_shift * identity
    norm_scale = 2.5 / jnp.sqrt(jnp.sum(shifted * shifted, keepdims=True))
    moment = norm_scale * shifted
    for number in range(ITERS):
        factor = (5.0 * identity - moment) * 0.25
        factor_low = factor.astype(jnp.bfloat16)
        if number == 0:
            current = jnp.sqrt(jnp.sqrt(norm_scale)) * factor
        else:
            current = product(current.astype(jnp.bfloat16), factor_low)
        if number + 1 < ITERS:
            square = product(factor_low, factor_low).astype(jnp.bfloat16)
            fourth = product(square, square).astype(jnp.bfloat16)
            moment = product(fourth, moment.astype(jnp.bfloat16))
    return current.astype(jnp.bfloat16)


def product(left, right, dims=((1,), (0,))):
    return lax.dot_general(left, right, (dims, ((), ())), preferred_element_type=jnp.float32)


def finish(place, owned, left, right, stats, right_out, direction, fresh_left, left_now, updated):
    blocks, order = owned.shape[0], owned.shape[1]
    right_out[...] = right[...]
    left_now[...] = left[...]

    @pl.when(place[0] == 0)
    def _():
        fresh_left[...] = jnp.zeros(fresh_left.shape, fresh_left.dtype)

    @pl.when(place[0] == 1)
    def _():
        slot = place[1]
        block = owned[slot]
        updated[0] = decay_rate * stats[0] + product(block, block, ((1,), (1,))) / order
        updated[1] = decay_rate * stats[1] + product(block, block, ((0,), (0,))) / order

        def renew(side, carry):
            root = inverse_root(updated[side])

            @pl.when(side == 0)
            def _():
                left_now[slot] = root
                fresh_left[...] = root

            @pl.when(side == 1)
            def _():
                right_out[slot] = root

            return carry

        lax.fori_loop(0, 2, renew, 0)

    def step(k, carry):
        half = product(left_now[k], owned[k]).astype(jnp.bfloat16)
        direction[k] = product(half, right_out[k]).astype(jnp.bfloat16)
        return carry

    lax.fori_loop(0, blocks, step, 0)


def body(grads, owner_slot, refresh, left_stat, right_stat, left_root, right_root):
    blocks, order = grads.shape[1], grads.shape[2]
    xs = lax.axis_size("x")
    shards = lax.axis_size("shard")
    rows = order // (xs * FAR * NEAR)
    rep_index = lax.axis_index(REP)
    shard_index = lax.axis_index("shard")
    f32, bf16 = jnp.float32, jnp.bfloat16

    fresh_slot = owner_slot[refresh[0]]
    holder = fresh_slot // blocks
    slot_index = fresh_slot % blocks
    owns_fresh = holder == shard_index

    early = jnp.concatenate(
        [
            left_root,
            *in_halves(lax.dynamic_slice_in_dim(left_stat, slot_index, 1, 0)),
            *in_halves(lax.dynamic_slice_in_dim(right_stat, slot_index, 1, 0)),
        ]
    )
    entries = early.shape[0]
    early = jnp.broadcast_to(early.reshape(1, entries * rows, order), (xs, entries * rows, order))

    depth = order // xs
    parts = grads[0].reshape(blocks, xs, depth, order).transpose(1, 0, 2, 3)
    parts = jnp.concatenate([parts.reshape(xs, blocks * depth, order), early], axis=1)
    parts = exchange(lax.optimization_barrier(parts), "x")
    early = parts[:, blocks * depth :].reshape(xs, entries, rows, order)
    early = lax.all_gather(early, Z)
    parts = parts[:, : blocks * depth].astype(f32)
    partial = parts[0] + parts[1] + parts[2] + parts[3]
    partial = partial.reshape(blocks, FAR, NEAR, rows, order).transpose(2, 0, 1, 3, 4)
    partial = jnp.sum(exchange(partial, "near"), axis=0)
    partial = jnp.sum(exchange(partial.transpose(1, 0, 2, 3), "far"), axis=0)
    row_share = partial.astype(bf16)

    slot_table = owner_slot.reshape(shards, blocks)
    own_slots = lax.dynamic_index_in_dim(slot_table, shard_index, 0, keepdims=False)
    targets = own_slots // blocks
    selector = (targets[None, :] == jnp.arange(shards, dtype=jnp.int32)[:, None]).astype(bf16)
    outgoing = jnp.einsum("ok,krc->orc", selector, row_share, preferred_element_type=f32)
    incoming = exchange(outgoing.astype(bf16), "shard")
    wanted = shard_index * blocks + jnp.arange(blocks, dtype=jnp.int32)
    receiver = (jnp.transpose(slot_table) == wanted[:, None]).astype(bf16)
    owned_rows = jnp.einsum("ks,src->krc", receiver, incoming, preferred_element_type=f32)
    owned_rows = owned_rows.astype(bf16)

    gathered = spread(spread(spread(owned_rows, "far"), "near"), "x")
    gathered = gathered.transpose(3, 0, 2, 1, 4, 5).reshape(blocks, order, order)

    left_new = (
        decay_rate * left_stat
        + jnp.einsum("krc,kjc->krj", owned_rows, gathered, preferred_element_type=f32) / order
    )
    column_share = lax.dynamic_slice_in_dim(gathered, rep_index * rows, rows, 2)
    right_new = (
        decay_rate * right_stat
        + jnp.einsum("kic,kij->kcj", column_share, gathered, preferred_element_type=f32) / order
    )

    stats = early[:, :, blocks:].astype(f32)
    stats = stats.reshape(*stats.shape[:2], 2, 2, rows, order)
    stats = stats[:, :, :, 0] + stats[:, :, :, 1]
    stats = stats.transpose(2, 1, 0, 3, 4).reshape(2, order, order)
    left_whole = early[:, :, :blocks].transpose(2, 1, 0, 3, 4).reshape(blocks, order, order)

    place = jnp.stack([owns_fresh.astype(jnp.int32), slot_index.astype(jnp.int32)])
    whole = jax.ShapeDtypeStruct((blocks, order, order), bf16)
    right_root_new, direction, fresh_left = pl.pallas_call(
        finish,
        out_shape=(whole, whole, jax.ShapeDtypeStruct((order, order), bf16)),
        in_specs=[pl.BlockSpec(memory_space=pltpu.SMEM)]
        + [pl.BlockSpec(memory_space=pltpu.VMEM)] * 4,
        out_specs=[pl.BlockSpec(memory_space=pltpu.VMEM)] * 3,
        scratch_shapes=[
            pltpu.VMEM((blocks, order, order), bf16),
            pltpu.VMEM((2, order, order), f32),
        ],
    )(place, gathered, left_whole, right_root, stats)
    rows_x = lax.dynamic_slice_in_dim(fresh_left, rep_index * rows, rows, 0)
    renewed = lax.dynamic_update_index_in_dim(left_root, rows_x, slot_index, 0)
    left_root_new = jnp.where(owns_fresh, renewed, left_root)
    return (left_new, right_new, left_root_new, right_root_new, direction)


def solution(mesh):
    shards = mesh.shape["shard"]
    finer = Mesh(mesh.devices.reshape(-1, FAR, NEAR, shards), (*REP, "shard"))
    whole = P("shard", None, None)
    split = P("shard", REP, None)
    in_specs = (P(REP, "shard", None, None), P(), P(), split, split, split, whole)
    out_specs = (split, split, split, whole, whole)
    return jax.shard_map(body, mesh=finer, in_specs=in_specs, out_specs=out_specs, check_vma=False)
```

```python
import jax
import jax.numpy as jnp
from jax import lax
from jax.experimental import pallas as pl
from jax.experimental.pallas import tpu as pltpu
from jax.sharding import Mesh
from jax.sharding import PartitionSpec as P

ITERS = 2
FAR, NEAR = 8, 4
Z = ("far", "near")
REP = ("x",) + Z

decay_rate = 0.95
epsilon_shift = 1e-06


def exchange(blocks, axis):
    return lax.all_to_all(blocks, axis, split_axis=0, concat_axis=0, tiled=True)


def spread(piece, axis):
    copies = jnp.broadcast_to(piece[None], (lax.axis_size(axis), *piece.shape))
    return exchange(lax.optimization_barrier(copies), axis)


def in_halves(wide):
    high = lax.reduce_precision(wide, 8, 7)
    return [part.astype(jnp.bfloat16) for part in (high, wide - high)]


def inverse_root(statistic):
    order = statistic.shape[0]
    row = lax.broadcasted_iota(jnp.int32, statistic.shape, 0)
    column = lax.broadcasted_iota(jnp.int32, statistic.shape, 1)
    identity = (row == column).astype(jnp.float32)
    shifted = statistic + epsilon_shift * identity
    norm_scale = 2.5 / jnp.sqrt(jnp.sum(shifted * shifted, keepdims=True))
    moment = norm_scale * shifted
    for number in range(ITERS):
        factor = (5.0 * identity - moment) * 0.25
        factor_low = factor.astype(jnp.bfloat16)
        if number == 0:
            current = jnp.sqrt(jnp.sqrt(norm_scale)) * factor
        else:
            current = product(current.astype(jnp.bfloat16), factor_low)
        if number + 1 < ITERS:
            square = product(factor_low, factor_low).astype(jnp.bfloat16)
            fourth = product(square, square).astype(jnp.bfloat16)
            moment = product(fourth, moment.astype(jnp.bfloat16))
    return current.astype(jnp.bfloat16)


def product(left, right, dims=((1,), (0,))):
    return lax.dot_general(left, right, (dims, ((), ())), preferred_element_type=jnp.float32)


def finish(place, owned, early, right, right_out, direction, fresh_left, left_now, updated):
    blocks, order = owned.shape[0], owned.shape[1]
    depth, xs, _, rows, _ = early.shape
    tall, low = 16 // rows, 8 // rows
    right_out[...] = right[...]

    def unpack(i, carry):
        x, z = i // (depth // tall), i % (depth // tall) * tall
        place_at = pl.ds(pl.multiple_of(x * depth * rows + z * rows, 16), 16)
        for k in range(blocks):
            pieces = [early[z + j, x, k].astype(jnp.float32) for j in range(tall)]
            left_now[k, place_at] = jnp.concatenate(pieces, axis=0).astype(jnp.bfloat16)
        return carry

    lax.fori_loop(0, xs * depth // tall, unpack, 0)

    @pl.when(place[0] == 0)
    def _():
        fresh_left[...] = jnp.zeros(fresh_left.shape, fresh_left.dtype)

    @pl.when(place[0] == 1)
    def _():
        def unpack_stats(i, carry):
            x, z = i // (depth // low), i % (depth // low) * low
            place_at = pl.ds(pl.multiple_of(x * depth * rows + z * rows, 8), 8)
            for t in range(2):
                high = blocks + 2 * t
                pieces = [
                    early[z + j, x, high].astype(jnp.float32)
                    + early[z + j, x, high + 1].astype(jnp.float32)
                    for j in range(low)
                ]
                updated[t, place_at] = jnp.concatenate(pieces, axis=0)
            return carry

        lax.fori_loop(0, xs * depth // low, unpack_stats, 0)
        slot = place[1]
        block = owned[slot]
        updated[0] = decay_rate * updated[0] + product(block, block, ((1,), (1,))) / order
        updated[1] = decay_rate * updated[1] + product(block, block, ((0,), (0,))) / order

        def renew(side, carry):
            root = inverse_root(updated[side])

            @pl.when(side == 0)
            def _():
                left_now[slot] = root
                fresh_left[...] = root

            @pl.when(side == 1)
            def _():
                right_out[slot] = root

            return carry

        lax.fori_loop(0, 2, renew, 0)

    def step(k, carry):
        half = product(left_now[k], owned[k]).astype(jnp.bfloat16)
        direction[k] = product(half, right_out[k]).astype(jnp.bfloat16)
        return carry

    lax.fori_loop(0, blocks, step, 0)


def body(grads, owner_slot, refresh, left_stat, right_stat, left_root, right_root):
    blocks, order = grads.shape[1], grads.shape[2]
    xs = lax.axis_size("x")
    shards = lax.axis_size("shard")
    rows = order // (xs * FAR * NEAR)
    rep_index = lax.axis_index(REP)
    shard_index = lax.axis_index("shard")
    f32, bf16 = jnp.float32, jnp.bfloat16

    fresh_slot = owner_slot[refresh[0]]
    holder = fresh_slot // blocks
    slot_index = fresh_slot % blocks
    owns_fresh = holder == shard_index

    early = jnp.concatenate(
        [
            left_root,
            *in_halves(lax.dynamic_slice_in_dim(left_stat, slot_index, 1, 0)),
            *in_halves(lax.dynamic_slice_in_dim(right_stat, slot_index, 1, 0)),
        ]
    )
    entries = early.shape[0]
    early = jnp.broadcast_to(early.reshape(1, entries * rows, order), (xs, entries * rows, order))

    depth = order // xs
    parts = grads[0].reshape(blocks, xs, depth, order).transpose(1, 0, 2, 3)
    parts = jnp.concatenate([parts.reshape(xs, blocks * depth, order), early], axis=1)
    parts = exchange(lax.optimization_barrier(parts), "x")
    early = parts[:, blocks * depth :].reshape(xs, entries, rows, order)
    early = lax.all_gather(early, Z)
    parts = parts[:, : blocks * depth].astype(f32)
    partial = parts[0] + parts[1] + parts[2] + parts[3]
    partial = partial.reshape(blocks, FAR, NEAR, rows, order).transpose(2, 0, 1, 3, 4)
    partial = jnp.sum(exchange(partial, "near"), axis=0)
    partial = jnp.sum(exchange(partial.transpose(1, 0, 2, 3), "far"), axis=0)
    row_share = partial.astype(bf16)

    slot_table = owner_slot.reshape(shards, blocks)
    own_slots = lax.dynamic_index_in_dim(slot_table, shard_index, 0, keepdims=False)
    targets = own_slots // blocks
    selector = (targets[None, :] == jnp.arange(shards, dtype=jnp.int32)[:, None]).astype(bf16)
    outgoing = jnp.einsum("ok,krc->orc", selector, row_share, preferred_element_type=f32)
    incoming = exchange(outgoing.astype(bf16), "shard")
    wanted = shard_index * blocks + jnp.arange(blocks, dtype=jnp.int32)
    receiver = (jnp.transpose(slot_table) == wanted[:, None]).astype(bf16)
    owned_rows = jnp.einsum("ks,src->krc", receiver, incoming, preferred_element_type=f32)
    owned_rows = owned_rows.astype(bf16)

    gathered = spread(spread(spread(owned_rows, "far"), "near"), "x")
    gathered = gathered.transpose(3, 0, 2, 1, 4, 5).reshape(blocks, order, order)

    left_new = (
        decay_rate * left_stat
        + jnp.einsum("krc,kjc->krj", owned_rows, gathered, preferred_element_type=f32) / order
    )
    column_share = lax.dynamic_slice_in_dim(gathered, rep_index * rows, rows, 2)
    right_new = (
        decay_rate * right_stat
        + jnp.einsum("kic,kij->kcj", column_share, gathered, preferred_element_type=f32) / order
    )

    place = jnp.stack([owns_fresh.astype(jnp.int32), slot_index.astype(jnp.int32)])
    whole = jax.ShapeDtypeStruct((blocks, order, order), bf16)
    right_root_new, direction, fresh_left = pl.pallas_call(
        finish,
        out_shape=(whole, whole, jax.ShapeDtypeStruct((order, order), bf16)),
        in_specs=[pl.BlockSpec(memory_space=pltpu.SMEM)]
        + [pl.BlockSpec(memory_space=pltpu.VMEM)] * 3,
        out_specs=[pl.BlockSpec(memory_space=pltpu.VMEM)] * 3,
        scratch_shapes=[
            pltpu.VMEM((blocks, order, order), bf16),
            pltpu.VMEM((2, order, order), f32),
        ],
    )(place, gathered, early, right_root)
    rows_x = lax.dynamic_slice_in_dim(fresh_left, rep_index * rows, rows, 0)
    renewed = lax.dynamic_update_index_in_dim(left_root, rows_x, slot_index, 0)
    left_root_new = jnp.where(owns_fresh, renewed, left_root)
    return (left_new, right_new, left_root_new, right_root_new, direction)


def solution(mesh):
    shards = mesh.shape["shard"]
    finer = Mesh(mesh.devices.reshape(-1, FAR, NEAR, shards), (*REP, "shard"))
    whole = P("shard", None, None)
    split = P("shard", REP, None)
    in_specs = (P(REP, "shard", None, None), P(), P(), split, split, split, whole)
    out_specs = (split, split, split, whole, whole)
    return jax.shard_map(body, mesh=finer, in_specs=in_specs, out_specs=out_specs, check_vma=False)
```

```python
import jax
import jax.numpy as jnp
from jax import lax
from jax.experimental import pallas as pl
from jax.experimental.pallas import tpu as pltpu
from jax.sharding import Mesh
from jax.sharding import PartitionSpec as P

ITERS = 2
FAR, NEAR = 4, 8
Z = ("far", "near")
REP = ("x",) + Z

decay_rate = 0.95
epsilon_shift = 1e-06


def exchange(blocks, axis):
    return lax.all_to_all(blocks, axis, split_axis=0, concat_axis=0, tiled=True)


def spread(piece, axis):
    copies = jnp.broadcast_to(piece[None], (lax.axis_size(axis), *piece.shape))
    return exchange(lax.optimization_barrier(copies), axis)


def in_halves(wide):
    high = lax.reduce_precision(wide, 8, 7)
    return [part.astype(jnp.bfloat16) for part in (high, wide - high)]


def inverse_root(statistic):
    order = statistic.shape[0]
    row = lax.broadcasted_iota(jnp.int32, statistic.shape, 0)
    column = lax.broadcasted_iota(jnp.int32, statistic.shape, 1)
    identity = (row == column).astype(jnp.float32)
    shifted = statistic + epsilon_shift * identity
    norm_scale = 2.5 / jnp.sqrt(jnp.sum(shifted * shifted, keepdims=True))
    moment = norm_scale * shifted
    for number in range(ITERS):
        factor = (5.0 * identity - moment) * 0.25
        factor_low = factor.astype(jnp.bfloat16)
        if number == 0:
            current = jnp.sqrt(jnp.sqrt(norm_scale)) * factor
        else:
            current = product(current.astype(jnp.bfloat16), factor_low)
        if number + 1 < ITERS:
            square = product(factor_low, factor_low).astype(jnp.bfloat16)
            fourth = product(square, square).astype(jnp.bfloat16)
            moment = product(fourth, moment.astype(jnp.bfloat16))
    return current.astype(jnp.bfloat16)


def product(left, right, dims=((1,), (0,))):
    return lax.dot_general(left, right, (dims, ((), ())), preferred_element_type=jnp.float32)


def finish(place, owned, early, right, right_out, direction, fresh_left, left_now, updated):
    blocks, order = owned.shape[0], owned.shape[1]
    depth, xs, _, rows, _ = early.shape
    tall, low = 16 // rows, 8 // rows
    right_out[...] = right[...]

    def unpack(i, carry):
        x, z = i // (depth // tall), i % (depth // tall) * tall
        place_at = pl.ds(pl.multiple_of(x * depth * rows + z * rows, 16), 16)
        for k in range(blocks):
            pieces = [early[z + j, x, k].astype(jnp.float32) for j in range(tall)]
            left_now[k, place_at] = jnp.concatenate(pieces, axis=0).astype(jnp.bfloat16)
        return carry

    lax.fori_loop(0, xs * depth // tall, unpack, 0)

    @pl.when(place[0] == 0)
    def _():
        fresh_left[...] = jnp.zeros(fresh_left.shape, fresh_left.dtype)

    @pl.when(place[0] == 1)
    def _():
        def unpack_stats(i, carry):
            x, z = i // (depth // low), i % (depth // low) * low
            place_at = pl.ds(pl.multiple_of(x * depth * rows + z * rows, 8), 8)
            for t in range(2):
                high = blocks + 2 * t
                pieces = [
                    early[z + j, x, high].astype(jnp.float32)
                    + early[z + j, x, high + 1].astype(jnp.float32)
                    for j in range(low)
                ]
                updated[t, place_at] = jnp.concatenate(pieces, axis=0)
            return carry

        lax.fori_loop(0, xs * depth // low, unpack_stats, 0)
        slot = place[1]
        block = owned[slot]
        updated[0] = decay_rate * updated[0] + product(block, block, ((1,), (1,))) / order
        updated[1] = decay_rate * updated[1] + product(block, block, ((0,), (0,))) / order

        def renew(side, carry):
            root = inverse_root(updated[side])

            @pl.when(side == 0)
            def _():
                left_now[slot] = root
                fresh_left[...] = root

            @pl.when(side == 1)
            def _():
                right_out[slot] = root

            return carry

        lax.fori_loop(0, 2, renew, 0)

    def step(k, carry):
        half = product(left_now[k], owned[k]).astype(jnp.bfloat16)
        direction[k] = product(half, right_out[k]).astype(jnp.bfloat16)
        return carry

    lax.fori_loop(0, blocks, step, 0)


def body(grads, owner_slot, refresh, left_stat, right_stat, left_root, right_root):
    blocks, order = grads.shape[1], grads.shape[2]
    xs = lax.axis_size("x")
    shards = lax.axis_size("shard")
    rows = order // (xs * FAR * NEAR)
    rep_index = lax.axis_index(REP)
    shard_index = lax.axis_index("shard")
    f32, bf16 = jnp.float32, jnp.bfloat16

    fresh_slot = owner_slot[refresh[0]]
    holder = fresh_slot // blocks
    slot_index = fresh_slot % blocks
    owns_fresh = holder == shard_index

    early = jnp.concatenate(
        [
            left_root,
            *in_halves(lax.dynamic_slice_in_dim(left_stat, slot_index, 1, 0)),
            *in_halves(lax.dynamic_slice_in_dim(right_stat, slot_index, 1, 0)),
        ]
    )
    entries = early.shape[0]
    early = jnp.broadcast_to(early.reshape(1, entries * rows, order), (xs, entries * rows, order))

    depth = order // xs
    parts = grads[0].reshape(blocks, xs, depth, order).transpose(1, 0, 2, 3)
    parts = jnp.concatenate([parts.reshape(xs, blocks * depth, order), early], axis=1)
    parts = exchange(lax.optimization_barrier(parts), "x")
    early = parts[:, blocks * depth :].reshape(xs, entries, rows, order)
    early = lax.all_gather(early, Z)
    parts = parts[:, : blocks * depth].astype(f32)
    partial = parts[0] + parts[1] + parts[2] + parts[3]
    partial = partial.reshape(blocks, FAR, NEAR, rows, order).transpose(2, 0, 1, 3, 4)
    partial = jnp.sum(exchange(partial, "near"), axis=0)
    partial = jnp.sum(exchange(partial.transpose(1, 0, 2, 3), "far"), axis=0)
    row_share = partial.astype(bf16)

    slot_table = owner_slot.reshape(shards, blocks)
    own_slots = lax.dynamic_index_in_dim(slot_table, shard_index, 0, keepdims=False)
    targets = own_slots // blocks
    selector = (targets[None, :] == jnp.arange(shards, dtype=jnp.int32)[:, None]).astype(bf16)
    outgoing = jnp.einsum("ok,krc->orc", selector, row_share, preferred_element_type=f32)
    incoming = exchange(outgoing.astype(bf16), "shard")
    wanted = shard_index * blocks + jnp.arange(blocks, dtype=jnp.int32)
    receiver = (jnp.transpose(slot_table) == wanted[:, None]).astype(bf16)
    owned_rows = jnp.einsum("ks,src->krc", receiver, incoming, preferred_element_type=f32)
    owned_rows = owned_rows.astype(bf16)

    gathered = spread(spread(spread(owned_rows, "far"), "near"), "x")
    gathered = gathered.transpose(3, 0, 2, 1, 4, 5).reshape(blocks, order, order)

    left_new = (
        decay_rate * left_stat
        + jnp.einsum("krc,kjc->krj", owned_rows, gathered, preferred_element_type=f32) / order
    )
    column_share = lax.dynamic_slice_in_dim(gathered, rep_index * rows, rows, 2)
    right_new = (
        decay_rate * right_stat
        + jnp.einsum("kic,kij->kcj", column_share, gathered, preferred_element_type=f32) / order
    )

    place = jnp.stack([owns_fresh.astype(jnp.int32), slot_index.astype(jnp.int32)])
    whole = jax.ShapeDtypeStruct((blocks, order, order), bf16)
    right_root_new, direction, fresh_left = pl.pallas_call(
        finish,
        out_shape=(whole, whole, jax.ShapeDtypeStruct((order, order), bf16)),
        in_specs=[pl.BlockSpec(memory_space=pltpu.SMEM)]
        + [pl.BlockSpec(memory_space=pltpu.VMEM)] * 3,
        out_specs=[pl.BlockSpec(memory_space=pltpu.VMEM)] * 3,
        scratch_shapes=[
            pltpu.VMEM((blocks, order, order), bf16),
            pltpu.VMEM((2, order, order), f32),
        ],
    )(place, gathered, early, right_root)
    rows_x = lax.dynamic_slice_in_dim(fresh_left, rep_index * rows, rows, 0)
    renewed = lax.dynamic_update_index_in_dim(left_root, rows_x, slot_index, 0)
    left_root_new = jnp.where(owns_fresh, renewed, left_root)
    return (left_new, right_new, left_root_new, right_root_new, direction)


def solution(mesh):
    shards = mesh.shape["shard"]
    finer = Mesh(mesh.devices.reshape(-1, FAR, NEAR, shards), (*REP, "shard"))
    whole = P("shard", None, None)
    split = P("shard", REP, None)
    in_specs = (P(REP, "shard", None, None), P(), P(), split, split, split, whole)
    out_specs = (split, split, split, whole, whole)
    return jax.shard_map(body, mesh=finer, in_specs=in_specs, out_specs=out_specs, check_vma=False)
```
